32 devices in a mesh: section: 2 (over x), dp: 16 (over z, y, core).
Axes of the slice: x: 2, y: 2, z: 4, core: 2. Of those that a mesh axis runs over, the one named last changes fastest.
Arguments:
- activations: bfloat16 [4, 256, 4608], P('section', 'dp'), may hold values from -6 to 6
- section_sources: int32 [4], replicated, may hold values from 0 to 3, as said below
- accumulators: float32 [256, 4, 4608], P('dp', 'section'), may hold values from -6 to 6
- block_sources: int32 [256], replicated, may hold values from 0 to 255, as said below
- loss_terms: float32 [2, 16], P('section', 'dp'), may hold values from 0.35 to 6
- pre_gain: float32 [2, 4608], P('section'), may hold values from 0.1 to 1.9
- query_weight: bfloat16 [2, 4608, 2048], P('section', None, 'dp'), may hold values from -0.09375 to 0.09375
- keyval_weight: bfloat16 [2, 4608, 2048], P('section', None, 'dp'), may hold values from -0.09375 to 0.09375
- output_weight: bfloat16 [2, 2048, 4608], P('section', 'dp'), may hold values from -0.125 to 0.125
- post_gain: float32 [2, 4608], P('section'), may hold values from 0.1 to 1.9
Outputs:
- new_activations: bfloat16 [4, 256, 4608], P('section', 'dp')
- new_accumulators: float32 [256, 4, 4608], P('dp', 'section')
- check_out: bfloat16 [2, 256, 4608], P('section', 'dp')
The draws below stay inside these ranges and needn't reach their ends.
Inputs may be any that keep to these rules, and one draw needn't show every extreme that they name: `section_sources`: A permutation; each old section's micro-batches fill 1 slots of each new section. `block_sources`: A permutation; each old data index's blocks fill 1 block of each new data index.
All inputs are finite; a program needn't handle non-finite values.
Results may differ from the reference program's by a relative error of at most 0.014.
Values may be sent and summed in bfloat16 or wider, within the bound.
A program may use at most 64 MiB of HBM per device.

```python
import jax
import jax.numpy as jnp
from jax import lax

D = 4608
HD = 128
HEADS = 16
KV_HEADS = 8
TOKENS = 256
MB_DEV = 2
MB_ALL = 4
BROWS = 2
BLK_DEV = 16
BLOCKS = 256
ACC_ROWS = 4
N_SECTION = 2
N_DP = 16


def balanced_sources(key, groups, per_group):
    per_peer = per_group // groups

    def source_order(which):
        return jax.random.permutation(jax.random.fold_in(key, which), per_group)
    orders = jax.vmap(source_order)(jnp.arange(groups, dtype=jnp.int32))
    sources = jnp.arange(groups, dtype=jnp.int32)[:, None] * per_group + orders.astype(jnp.int32)
    chosen = sources.reshape(groups, groups, per_peer).transpose(1, 0, 2).reshape(groups, per_group)

    def shuffle(which, entries):
        return jax.random.permutation(jax.random.fold_in(key, 100000 + which), entries)
    table = jax.vmap(shuffle)(jnp.arange(groups, dtype=jnp.int32), chosen)
    return table.reshape(-1).astype(jnp.int32)


def draw_section_sources(key, part):
    return balanced_sources(jax.random.fold_in(key, 11), N_SECTION, MB_DEV)


def draw_block_sources(key, part):
    return balanced_sources(jax.random.fold_in(key, 23), N_DP, BLK_DEV)


def draw_loss_terms(key, part):
    rising = 1.0 + 2.0 * jnp.arange(N_DP, dtype=jnp.float32) / (N_DP - 1)
    subkey = jax.random.fold_in(key, 37)
    factor = jnp.exp(jax.random.uniform(subkey, (N_SECTION, N_DP), jnp.float32, jnp.log(0.7), jnp.log(1.4)))
    return (rising[None, :] * factor).astype(jnp.float32)


def shard_levels(stream_key, extent, shards, smallest, top_value):
    loudness, own = 1.0, jax.random.fold_in(stream_key, 6)
    for axis_at, blocks in shards:
        steps = jnp.exp(jax.random.uniform(jax.random.fold_in(own, axis_at), (blocks,), jnp.float32, smallest / len(shards), top_value / len(shards)))
        loudness = loudness * jnp.repeat(steps, extent[axis_at] // blocks).reshape([-1 if axis == axis_at else 1 for axis in range(len(extent))])
    return loudness


def bell_draw(rng, extent, spread, reach, shards=(), held_as=jnp.bfloat16):
    values = jax.random.normal(rng, extent, jnp.float32) * spread
    if len(shards) > 0:
        values = shard_levels(rng, extent, shards, -0.22, 0.18) * values
    return jnp.clip(values, min=-reach, max=reach).astype(held_as)


def setup_inputs(seed: int = 0) -> dict:
    seeds = jax.random.split(jax.random.key(seed), 11)
    activations = bell_draw(seeds[0], (MB_ALL, TOKENS, D), 1.0, 6.0, ((0, 2), (1, 16)))
    section_sources = draw_section_sources(jax.random.fold_in(seeds[10], 71), 0)
    accumulators = bell_draw(seeds[2], (BLOCKS, ACC_ROWS, D), 1.0, 6.0, ((0, 16), (1, 2)), jnp.float32)
    block_sources = draw_block_sources(jax.random.fold_in(seeds[10], 71), 0)
    loss_terms = draw_loss_terms(jax.random.fold_in(seeds[10], 71), 0)
    pre_gain = jnp.clip(1.0 + 0.18 * jax.random.normal(seeds[5], (N_SECTION, D), jnp.float32), 0.1, 1.9)
    query_weight = bell_draw(seeds[6], (N_SECTION, D, HEADS * HD), D ** -0.5, 0.09375, ((0, 2), (2, 16)))
    keyval_weight = bell_draw(seeds[7], (N_SECTION, D, HEADS * HD), D ** -0.5, 0.09375, ((0, 2), (2, 16)))
    output_weight = bell_draw(seeds[8], (N_SECTION, HEADS * HD, D), (HEADS * HD) ** -0.5, 0.125, ((0, 2), (1, 16)))
    post_gain = jnp.clip(1.0 + 0.18 * jax.random.normal(seeds[9], (N_SECTION, D), jnp.float32), 0.1, 1.9)
    return dict(activations=activations, section_sources=section_sources, accumulators=accumulators, block_sources=block_sources, loss_terms=loss_terms, pre_gain=pre_gain, query_weight=query_weight, keyval_weight=keyval_weight, output_weight=output_weight, post_gain=post_gain)


def rms_norm(values, gain):
    meansq = lax.optimization_barrier(jnp.mean(values * values, axis=-1, keepdims=True))
    return values * lax.rsqrt(meansq + 1e-06) * gain

def rotary(values, positions):
    width = values.shape[-1]
    middle = width // 2
    counter = jnp.arange(middle, dtype=jnp.float32)
    freqs = 10000.0 ** (-2.0 * counter / width)
    angles = positions.astype(jnp.float32)[:, None] * freqs[None, :]
    cosine = jnp.cos(angles)
    sine = jnp.sin(angles)
    if values.ndim == 3:
        cosine = cosine[:, None, :]
        sine = sine[:, None, :]
    first = values[..., :middle]
    second = values[..., middle:]
    return jnp.concatenate([first * cosine - second * sine, second * cosine + first * sine], axis=-1)

def check_layer(checked, gain_pre, w_query, w_keyval, w_output, gain_post):
    length = checked.shape[0]
    positions = jnp.arange(length, dtype=jnp.int32)
    normed = rms_norm(checked.astype(jnp.float32), gain_pre).astype(jnp.bfloat16)
    queries = jnp.dot(normed, w_query, preferred_element_type=jnp.float32).reshape(length, HEADS, HD)
    keyvals = jnp.dot(normed, w_keyval, preferred_element_type=jnp.float32).reshape(length, KV_HEADS, 2, HD)
    queries = rotary(queries, positions).astype(jnp.bfloat16)
    key_rows = rotary(keyvals[:, :, 0, :], positions).astype(jnp.bfloat16)
    value_rows = keyvals[:, :, 1, :].astype(jnp.bfloat16)
    key_rows = jnp.repeat(key_rows, 2, axis=1)
    value_rows = jnp.repeat(value_rows, 2, axis=1)
    scale_factor = (D / HEADS) ** (-0.5)
    scores = jnp.einsum('qhd,khd->hqk', queries.astype(jnp.float32), key_rows.astype(jnp.float32)) * scale_factor
    capped = 50.0 * jnp.tanh(scores / 50.0)
    causal = positions[None, :] <= positions[:, None]
    expd = jnp.where(causal[None, :, :], jnp.exp(capped), 0.0)
    denominator = lax.optimization_barrier(jnp.sum(expd, axis=-1))
    probs = expd.astype(jnp.bfloat16)
    numer = jnp.einsum('hqk,khd->hqd', probs.astype(jnp.float32), value_rows.astype(jnp.float32))
    attended = (numer / denominator[:, :, None]).astype(jnp.bfloat16)
    attended = jnp.transpose(attended, (1, 0, 2)).reshape(length, HEADS * HD)
    summed = jnp.dot(attended, w_output, preferred_element_type=jnp.float32)
    return (checked.astype(jnp.float32) + rms_norm(summed, gain_post)).astype(jnp.bfloat16)

def reference(activations, section_sources, accumulators, block_sources, loss_terms, pre_gain, query_weight, keyval_weight, output_weight, post_gain):
    moved = jnp.take(activations, section_sources, axis=0)
    regrouped = jnp.take(accumulators, block_sources, axis=0)
    totals = lax.optimization_barrier(jnp.sum(loss_terms, axis=1))
    factor = N_DP / totals
    scaled = regrouped.reshape(BLOCKS, N_SECTION, BROWS, D) * factor[None, :, None, None]
    new_accumulators = scaled.reshape(BLOCKS, ACC_ROWS, D)
    checks = []
    for section_id in range(N_SECTION):
        checks.append(check_layer(moved[section_id * MB_DEV], pre_gain[section_id], query_weight[section_id], keyval_weight[section_id], output_weight[section_id], post_gain[section_id]))
    return (moved, new_accumulators, jnp.stack(checks, axis=0))
```

```python
import functools

import jax
import jax.numpy as jnp
import numpy as np
from jax import lax
from jax.experimental import pallas as pl
from jax.experimental.pallas import tpu as pltpu
from jax.sharding import PartitionSpec as P

LANES = 128
CHUNKS = 4
F32 = jnp.float32
BF16 = jnp.bfloat16


def routes(sources, own, groups, per_group):
    per_peer = per_group // groups
    table = sources.reshape(groups, per_group)
    owners = table // per_group
    places = table % per_group
    mine = owners == own
    my_owners = lax.dynamic_slice_in_dim(owners, own, 1, 0)[0]
    if per_peer == 1:
        send = jnp.sum(jnp.where(mine, places, 0), axis=1)
        return send, my_owners
    rank = jnp.cumsum(mine.astype(jnp.int32), axis=1) - 1
    picked = mine[:, None, :] & (rank[:, None, :] == jnp.arange(per_peer)[None, :, None])
    send = jnp.sum(jnp.where(picked, places[:, None, :], 0), axis=2).reshape(-1)
    ids = jnp.arange(per_group)
    earlier = (my_owners[None, :] == my_owners[:, None]) & (ids[None, :] < ids[:, None])
    return send, my_owners * per_peer + jnp.sum(earlier.astype(jnp.int32), axis=1)


def rotary_tables(length, width):
    half = width // 2
    freqs = np.float32(10000.0) ** (np.float32(-2.0) * np.arange(half, dtype=np.float32) / np.float32(width))
    angles = np.arange(length, dtype=np.float32)[:, None] * freqs.astype(np.float32)[None, :]
    cosine, sine = np.cos(angles.astype(np.float64)), np.sin(angles.astype(np.float64))
    return np.stack(
        [np.concatenate([cosine, cosine], 1), np.concatenate([-sine, sine], 1)]
    ).astype(np.float32)


def kernel(
    dims,
    act_send, act_recv, blk_send, blk_recv, loss,
    act_hbm, acc_hbm, pre_hbm, wq_hbm, wkv_hbm, wo_hbm, post_hbm, rot_hbm,
    moved_hbm, newacc_hbm, check_hbm,
    act, acc, pre, post, rot, w, wo,
    stage, actrecv, moved, sacc, racc, accout,
    gath, qkv, part, pair_in, ring_in, ring_out, outbuf,
    load_sem, store_sem, act_sem, w_sem, blk_sem, ag_sem, own_sem, fwd_sem, pair_sem, ring_sem,
):
    n_sec, n_dp = dims
    mb, toks, d = act.shape
    blk, brows, _ = acc.shape
    act_pp, blk_pp = mb // n_sec, blk // n_dp
    chips = n_dp // 2
    far = chips // 2
    kd = d // CHUNKS
    length = n_dp * toks
    hd = wq_hbm.shape[2]
    sec, me = lax.axis_index("section"), lax.axis_index("dp")
    core, chip = me % 2, me // 2
    side, rung = chip % 2, chip // 2
    pos = rung * (1 - side) + (chips - 1 - rung) * side

    def chip_at(p):
        q = (p + 2 * chips) % chips
        s = q // (chips // 2)
        return 2 * (q * (1 - s) + (chips - 1 - q) * s) + s

    def device(p):
        return {"dp": 2 * chip_at(p) + core}

    partner = {"dp": me + 1 - 2 * core}

    def remote(src, dst, sems, dev):
        return pltpu.make_async_remote_copy(
            src_ref=src, dst_ref=dst, send_sem=sems.at[0], recv_sem=sems.at[1],
            device_id=dev, device_id_type=pl.DeviceIdType.MESH,
        )

    barrier = pltpu.get_barrier_semaphore()
    for o in range(1, n_sec):
        pl.semaphore_signal(barrier, inc=1, device_id={"section": (sec + o) % n_sec},
                            device_id_type=pl.DeviceIdType.MESH)
    for o in range(1, n_dp):
        pl.semaphore_signal(barrier, inc=1, device_id={"dp": (me + o) % n_dp},
                            device_id_type=pl.DeviceIdType.MESH)

    kv_cols = pl.ds(pl.multiple_of(hd + core * hd, LANES), hd)
    loads = [
        pltpu.make_async_copy(src, dst, load_sem.at[i])
        for i, (src, dst) in enumerate([
            (act_hbm, act), (wkv_hbm.at[0], w.at[:, kv_cols]), (pre_hbm, pre), (acc_hbm, acc),
            (wq_hbm.at[0], w.at[:, pl.ds(0, hd)]), (rot_hbm, rot), (wo_hbm.at[0], wo), (post_hbm, post),
        ])
    ]
    for load in loads:
        load.start()

    loads[0].wait()
    for q in range(n_sec):
        for r in range(act_pp):
            stage[q, r] = act[act_send[q * act_pp + r]]
    pl.semaphore_wait(barrier, n_sec - 1 + n_dp - 1)
    act_copies = []
    for o in range(1, n_sec):
        q = (sec + o) % n_sec
        copy = remote(stage.at[q], actrecv.at[sec], act_sem.at[o - 1], {"section": q})
        copy.start()
        act_copies.append(copy)
    actrecv[sec] = stage[sec]

    loads[1].wait()
    kv_copy = remote(w.at[:, kv_cols], w.at[:, kv_cols], w_sem, partner)
    kv_copy.start()

    loads[3].wait()
    term = jnp.full((brows, LANES), loss[0, 0], F32)
    high = term.astype(BF16).astype(F32)
    row = lax.broadcasted_iota(jnp.int32, (brows, LANES), 0)
    tail = jnp.where(row == 0, high, jnp.where(row == 1, term - high, 0.0)).astype(BF16)

    def pack(p, carry):
        for r in range(blk_pp):
            sacc[p, r, :, pl.ds(0, d)] = acc[blk_send[p * blk_pp + r]].astype(BF16)
            sacc[p, r, :, pl.ds(d, LANES)] = tail
        return carry

    lax.fori_loop(0, n_dp, pack, 0)
    racc[me] = sacc[me]

    loads[2].wait()
    for copy in act_copies:
        copy.wait_recv()
    for j in range(mb):
        src = act_recv[j]
        moved[j] = actrecv[src // act_pp, src % act_pp] if act_pp > 1 else actrecv[src, 0]
    checked = moved[0].astype(F32)
    normed = checked * lax.rsqrt(jnp.mean(checked * checked, axis=-1, keepdims=True) + 1e-06)
    normed = (normed * pre[...]).astype(BF16)
    for k in range(CHUNKS):
        gath[k, me] = normed[:, k * kd:(k + 1) * kd]
    stores = [pltpu.make_async_copy(moved, moved_hbm, store_sem.at[0])]
    stores[0].start()

    def hops(way, k):
        return far if (k < CHUNKS // 2) == (way == 0) else far - 1

    step_of = (1, -1)
    sent = []

    def gather_copy(way, hop, k, source):
        block = gath.at[k, source]
        return remote(block, block, ag_sem.at[way, hop - 1, k], device(pos + step_of[way]))

    def pass_on(source, k, sems):
        block = gath.at[k, source]
        copy = remote(block, block, sems, partner)
        copy.start()
        sent.append(copy)

    for k in range(CHUNKS):
        for way in range(2):
            copy = gather_copy(way, 1, k, me)
            copy.start()
            sent.append(copy)
    for k in range(CHUNKS):
        pass_on(me, k, own_sem.at[k])
    for hop in range(1, far + 1):
        for k in range(CHUNKS):
            for way in range(2):
                if hop > hops(way, k):
                    continue
                source = 2 * chip_at(pos - step_of[way] * hop) + core
                gather_copy(way, hop, k, source).wait_recv()
                if hop < hops(way, k):
                    copy = gather_copy(way, hop + 1, k, source)
                    copy.start()
                    sent.append(copy)
                pass_on(source, k, fwd_sem.at[way, hop - 1, k])

    blk_copies = []
    for o in range(1, n_dp):
        peer = (me + o) % n_dp
        copy = remote(sacc.at[peer], racc.at[me], blk_sem.at[o - 1], {"dp": peer})
        copy.start()
        blk_copies.append(copy)

    kv_copy.wait_recv()
    loads[4].wait()
    other = me + 1 - 2 * core
    for k in range(CHUNKS):
        remote(gath.at[k, other], gath.at[k, other], own_sem.at[k], partner).wait_recv()
    for hop in range(1, far + 1):
        for k in range(CHUNKS):
            for way in range(2):
                if hop <= hops(way, k):
                    source = 2 * chip_at(pos - step_of[way] * hop) + 1 - core
                    block = gath.at[k, source]
                    remote(block, block, fwd_sem.at[way, hop - 1, k], partner).wait_recv()

    qkv[...] = jnp.zeros_like(qkv)

    def project(k, carry):
        rows = gath[k].reshape(length, kd)
        cols = w[pl.ds(pl.multiple_of(k * kd, LANES), kd), :]
        qkv[...] += jnp.dot(rows, cols, preferred_element_type=F32)
        return carry

    lax.fori_loop(0, CHUNKS, project, 0)
    loads[5].wait()
    cosine, sine = rot[0], rot[1]

    def turned(v):
        return (v * cosine + pltpu.roll(v, hd // 2, 1) * sine).astype(BF16)

    queries = turned(qkv[:, 0:hd])
    keys = turned(qkv[:, hd:2 * hd])
    values = qkv[:, 2 * hd:3 * hd].astype(BF16)
    scores = lax.dot_general(queries, keys, (((1,), (1,)), ((), ())), preferred_element_type=F32)
    scores = scores * ((d / n_dp) ** (-0.5) / 50.0)
    at_query = lax.broadcasted_iota(jnp.int32, scores.shape, 0)
    at_key = lax.broadcasted_iota(jnp.int32, scores.shape, 1)
    expd = jnp.where(at_key <= at_query, jnp.exp(50.0 * jnp.tanh(scores)), 0.0)
    denominator = jnp.sum(expd, axis=-1, keepdims=True)
    numer = jnp.dot(expd.astype(BF16), values, preferred_element_type=F32)
    attended = (numer / denominator).astype(BF16)

    loads[6].wait()
    pair_copies = []
    for k in range(CHUNKS):
        terms = jnp.dot(attended, wo[:, k * kd:(k + 1) * kd], preferred_element_type=F32).astype(BF16)
        part[k] = terms.reshape(chips, 2, toks, kd)
        copy = remote(part.at[k, :, 1 - core], pair_in.at[k], pair_sem.at[k], partner)
        copy.start()
        pair_copies.append(copy)

    def own_terms(k, p):
        target = chip_at(p)
        return part[k, target, core].astype(F32) + pair_in[k, target].astype(F32)

    def ring_copy(way, step, k):
        return remote(ring_out.at[way, step - 1, k], ring_in.at[way, step - 1, k],
                      ring_sem.at[way, step - 1, k], device(pos + step_of[way]))

    for k in range(CHUNKS):
        pair_copies[k].wait_recv()
        for way in range(2):
            ring_out[way, 0, k] = own_terms(k, pos + step_of[way] * hops(way, k)).astype(BF16)
            copy = ring_copy(way, 1, k)
            copy.start()
            sent.append(copy)
    for step in range(1, far):
        for k in range(CHUNKS):
            for way in range(2):
                left = hops(way, k) - step
                if left < 1:
                    continue
                ring_copy(way, step, k).wait_recv()
                total = own_terms(k, pos + step_of[way] * left) + ring_in[way, step - 1, k].astype(F32)
                ring_out[way, step, k] = total.astype(BF16)
                copy = ring_copy(way, step + 1, k)
                copy.start()
                sent.append(copy)

    for copy in blk_copies:
        copy.wait_recv()
    scale_sum = jnp.sum(jnp.sum(racc[:, 0, :, pl.ds(d, LANES)].astype(F32), axis=0), axis=0, keepdims=True)
    factor = (n_dp / scale_sum)[:, 0:1]

    def unpack(b, carry):
        src = blk_recv[b]
        if blk_pp > 1:
            block = racc[src // blk_pp, src % blk_pp, :, pl.ds(0, d)]
        else:
            block = racc[src, 0, :, pl.ds(0, d)]
        accout[b] = block.astype(F32) * factor
        return carry

    lax.fori_loop(0, blk, unpack, 0)
    stores.append(pltpu.make_async_copy(accout, newacc_hbm, store_sem.at[1]))
    stores[1].start()

    pieces = []
    for k in range(CHUNKS):
        total = own_terms(k, pos)
        for way in range(2):
            step = hops(way, k)
            ring_copy(way, step, k).wait_recv()
            total = total + ring_in[way, step - 1, k].astype(F32)
        pieces.append(total)
    loads[7].wait()
    square = sum(jnp.sum(t * t, axis=-1, keepdims=True) for t in pieces)
    scale = lax.rsqrt(square / d + 1e-06)
    for k in range(CHUNKS):
        cols = slice(k * kd, (k + 1) * kd)
        outbuf[0, :, cols] = (
            moved[0, :, cols].astype(F32) + pieces[k] * scale * post[:, cols]
        ).astype(BF16)
    stores.append(pltpu.make_async_copy(outbuf, check_hbm, store_sem.at[2]))
    stores[2].start()

    for copy in act_copies + [kv_copy] + sent + blk_copies + pair_copies:
        copy.wait_send()
    for store in stores:
        store.wait()


def make_on_device(n_sec, n_dp):
    def on_device(activations, section_sources, accumulators, block_sources, loss_terms,
                  pre_gain, query_weight, keyval_weight, output_weight, post_gain):
        mb, toks, d = activations.shape
        blk, brows, _ = accumulators.shape
        hd = query_weight.shape[2]
        chips, far, kd, length = n_dp // 2, n_dp // 4, d // CHUNKS, n_dp * toks
        act_send, act_recv = routes(section_sources, lax.axis_index("section"), n_sec, mb)
        blk_send, blk_recv = routes(block_sources, lax.axis_index("dp"), n_dp, blk)
        rot = jnp.asarray(rotary_tables(length, hd))
        smem = pl.BlockSpec(memory_space=pltpu.SMEM)
        anywhere = pl.BlockSpec(memory_space=pl.ANY)
        dma = pltpu.SemaphoreType.DMA
        act_pp, blk_pp = mb // n_sec, blk // n_dp

        return pl.pallas_call(
            functools.partial(kernel, (n_sec, n_dp)),
            out_shape=(
                jax.ShapeDtypeStruct(activations.shape, BF16),
                jax.ShapeDtypeStruct(accumulators.shape, F32),
                jax.ShapeDtypeStruct((1, toks, d), BF16),
            ),
            in_specs=[smem] * 5 + [anywhere] * 8,
            out_specs=(anywhere,) * 3,
            scratch_shapes=[
                pltpu.VMEM(activations.shape, BF16),
                pltpu.VMEM(accumulators.shape, F32),
                pltpu.VMEM((1, d), F32),
                pltpu.VMEM((1, d), F32),
                pltpu.VMEM(rot.shape, F32),
                pltpu.VMEM((d, 3 * hd), BF16),
                pltpu.VMEM((hd, d), BF16),
                pltpu.VMEM((n_sec, act_pp, toks, d), BF16),
                pltpu.VMEM((n_sec, act_pp, toks, d), BF16),
                pltpu.VMEM(activations.shape, BF16),
                pltpu.VMEM((n_dp, blk_pp, brows, d + LANES), BF16),
                pltpu.VMEM((n_dp, blk_pp, brows, d + LANES), BF16),
                pltpu.VMEM(accumulators.shape, F32),
                pltpu.VMEM((CHUNKS, n_dp, toks, kd), BF16),
                pltpu.VMEM((length, 3 * hd), F32),
                pltpu.VMEM((CHUNKS, chips, 2, toks, kd), BF16),
                pltpu.VMEM((CHUNKS, chips, toks, kd), BF16),
                pltpu.VMEM((2, far, CHUNKS, toks, kd), BF16),
                pltpu.VMEM((2, far, CHUNKS, toks, kd), BF16),
                pltpu.VMEM((1, toks, d), BF16),
                dma((8,)),
                dma((3,)),
                dma((n_sec - 1, 2)),
                dma((2,)),
                dma((n_dp - 1, 2)),
                dma((2, far, CHUNKS, 2)),
                dma((CHUNKS, 2)),
                dma((2, far, CHUNKS, 2)),
                dma((CHUNKS, 2)),
                dma((2, far, CHUNKS, 2)),
            ],
            compiler_params=pltpu.CompilerParams(
                collective_id=0, has_side_effects=True, vmem_limit_bytes=60 * 2**20
            ),
        )(act_send, act_recv, blk_send, blk_recv, loss_terms, activations, accumulators,
          pre_gain, query_weight, keyval_weight, output_weight, post_gain, rot)

    return on_device


def solution(mesh):
    placed = (
        P("section", "dp", None),
        P(),
        P("dp", "section", None),
        P(),
        P("section", "dp"),
        P("section", None),
        P("section", None, "dp"),
        P("section", None, "dp"),
        P("section", "dp", None),
        P("section", None),
    )
    return jax.shard_map(
        make_on_device(mesh.shape["section"], mesh.shape["dp"]),
        mesh=mesh,
        in_specs=placed,
        out_specs=(P("section", "dp", None), P("dp", "section", None), P("section", "dp", None)),
        check_vma=False,
    )
```

```python
import functools

import jax
import jax.numpy as jnp
import numpy as np
from jax import lax
from jax.experimental import pallas as pl
from jax.experimental.pallas import tpu as pltpu
from jax.sharding import PartitionSpec as P

LANES = 128
VMEM_BYTES = 67043328
CHUNKS = 4
F32 = jnp.float32
BF16 = jnp.bfloat16


def pick(table, own, groups, per_group, peer, rank):
    def visit(j, carry):
        seen, found = carry
        source = table[peer * per_group + j]
        mine = (source // per_group == own).astype(jnp.int32)
        hit = mine * (seen == rank).astype(jnp.int32)
        return seen + mine, found + hit * (source % per_group)

    zero = jnp.int32(0)
    return lax.fori_loop(0, per_group, visit, (zero, zero), unroll=True)[1]


def origin(table, own, per_group, per_peer, entry):
    owner = table[own * per_group + entry] // per_group
    if per_peer == 1:
        return owner, 0

    def visit(j, seen):
        same = table[own * per_group + j] // per_group == owner
        return seen + same.astype(jnp.int32) * (j < entry).astype(jnp.int32)

    return owner, lax.fori_loop(0, per_group, visit, jnp.int32(0))


def rotary_tables(length, width):
    half = width // 2
    freqs = np.float32(10000.0) ** (np.float32(-2.0) * np.arange(half, dtype=np.float32) / np.float32(width))
    angles = np.arange(length, dtype=np.float32)[:, None] * freqs.astype(np.float32)[None, :]
    cosine, sine = np.cos(angles.astype(np.float64)), np.sin(angles.astype(np.float64))
    return np.stack(
        [np.concatenate([cosine, cosine], 1), np.concatenate([-sine, sine], 1)]
    ).astype(np.float32)


def kernel(
    dims,
    secs_hbm, blks_hbm, loss_hbm, act_hbm, acc_hbm, pre_hbm, wq_hbm, wkv_hbm, wo_hbm, post_hbm, rot_hbm,
    moved, accout, outbuf,
    secs, blks, loss, act, acc, pre, post, rot, w, wo,
    stage, actrecv, sacc, racc,
    gath, qkv, att, att_in, part, ring_in, ring_out,
    load_sem, act_sem, w_sem, wo_sem, blk_sem, ag_sem, own_sem, fwd_sem, att_sem, ring_sem,
):
    n_sec, n_dp = dims
    mb, toks, d = act.shape
    blk, brows, _ = acc.shape
    act_pp, blk_pp = mb // n_sec, blk // n_dp
    chips = n_dp // 2
    far = chips // 2
    kd = d // CHUNKS
    length = n_dp * toks
    hd = wq_hbm.shape[2]
    sec, me = lax.axis_index("section"), lax.axis_index("dp")
    core, chip = me % 2, me // 2
    side, rung = chip % 2, chip // 2
    pos = rung * (1 - side) + (chips - 1 - rung) * side

    def chip_at(p):
        q = (p + 2 * chips) % chips
        s = q // (chips // 2)
        return 2 * (q * (1 - s) + (chips - 1 - q) * s) + s

    def device(p):
        return {"dp": 2 * chip_at(p) + core}

    partner = {"dp": me + 1 - 2 * core}

    def remote(src, dst, sems, dev):
        return pltpu.make_async_remote_copy(
            src_ref=src, dst_ref=dst, send_sem=sems.at[0], recv_sem=sems.at[1],
            device_id=dev, device_id_type=pl.DeviceIdType.MESH,
        )

    barrier = pltpu.get_barrier_semaphore()
    for o in range(1, n_sec):
        pl.semaphore_signal(barrier, inc=1, device_id={"section": (sec + o) % n_sec},
                            device_id_type=pl.DeviceIdType.MESH)
    for o in range(1, n_dp):
        pl.semaphore_signal(barrier, inc=1, device_id={"dp": (me + o) % n_dp},
                            device_id_type=pl.DeviceIdType.MESH)

    kv_cols = pl.ds(pl.multiple_of(hd + core * hd, LANES), hd)
    q_cols = pl.ds(0, hd)
    wo_rows = pl.ds(pl.multiple_of(core * hd, LANES), hd)
    names = ("secs", "act", "pre", "wkv", "wo", "blks", "loss", "acc", "wq", "rot", "post")
    pairs = [
        (secs_hbm, secs), (act_hbm, act), (pre_hbm, pre), (wkv_hbm.at[0], w.at[:, kv_cols]),
        (wo_hbm.at[0], wo.at[wo_rows]), (blks_hbm, blks), (loss_hbm, loss), (acc_hbm, acc),
        (wq_hbm.at[0], w.at[:, q_cols]), (rot_hbm, rot), (post_hbm, post),
    ]
    loads = {
        name: pltpu.make_async_copy(src, dst, load_sem.at[i])
        for i, (name, (src, dst)) in enumerate(zip(names, pairs))
    }
    for name in names:
        loads[name].start()

    loads["secs"].wait()
    loads["act"].wait()
    for q in range(n_sec):
        for r in range(act_pp):
            block = act[pick(secs, sec, n_sec, mb, q, r)]
            for k in range(CHUNKS):
                stage[q, k, r] = block[:, k * kd:(k + 1) * kd]
    pl.semaphore_wait(barrier, n_sec - 1 + n_dp - 1)
    act_copies = [[] for _ in range(CHUNKS)]
    for k in range(CHUNKS):
        for o in range(1, n_sec):
            q = (sec + o) % n_sec
            copy = remote(stage.at[q, k], actrecv[k].at[sec], act_sem.at[o - 1, k], {"section": q})
            copy.start()
            act_copies[k].append(copy)
    for k in range(CHUNKS):
        actrecv[k][sec] = stage[sec, k]

    loads["wkv"].wait()
    kv_copy = remote(w.at[:, kv_cols], w.at[:, kv_cols], w_sem, partner)
    kv_copy.start()
    loads["wo"].wait()
    wo_copy = remote(wo.at[wo_rows], wo.at[wo_rows], wo_sem, partner)
    wo_copy.start()
    loads["pre"].wait()

    def hops(way, k):
        return far if (k < CHUNKS // 2) == (way == 0) else far - 1

    step_of = (1, -1)
    sent = []

    def width(k):
        return kd + LANES if k == CHUNKS - 1 else kd

    def block_of(k, source):
        return gath.at[k, source, :, pl.ds(0, width(k))]

    def gather_copy(way, hop, k, source):
        block = block_of(k, source)
        return remote(block, block, ag_sem.at[way, hop - 1, k], device(pos + step_of[way]))

    def hand_over(source, k, sems):
        block = block_of(k, source)
        return remote(block, block, sems, partner)

    def pass_on(source, k, sems):
        copy = hand_over(source, k, sems)
        copy.start()
        sent.append(copy)

    square = jnp.zeros((toks, 1), F32)
    for k in range(CHUNKS):
        for copy in act_copies[k]:
            copy.wait_recv()
        owner, number = origin(secs, sec, mb, act_pp, 0)
        piece = actrecv[k][owner, number].astype(F32)
        square = square + jnp.sum(piece * piece, axis=-1, keepdims=True)
        gath[k, me, :, pl.ds(0, kd)] = (piece * pre[:, k * kd:(k + 1) * kd]).astype(BF16)
        if k == CHUNKS - 1:
            root = jnp.broadcast_to(lax.rsqrt(square / d + 1e-06), (toks, LANES))
            high = root.astype(BF16).astype(F32)
            lane = lax.broadcasted_iota(jnp.int32, (toks, LANES), 1)
            gath[k, me, :, pl.ds(kd, LANES)] = jnp.where(
                lane == 0, high, jnp.where(lane == 1, root - high, 0.0)).astype(BF16)
        for way in range(2):
            copy = gather_copy(way, 1, k, me)
            copy.start()
            sent.append(copy)
        pass_on(me, k, own_sem.at[k])

    for name in ("acc", "blks", "loss"):
        loads[name].wait()
    term = jnp.full((brows, LANES), loss[0, 0], F32)
    high = term.astype(BF16).astype(F32)
    lane = lax.broadcasted_iota(jnp.int32, (brows, LANES), 1)
    row = lax.broadcasted_iota(jnp.int32, (brows, LANES), 0)
    tail = jnp.where(row > 0, 0.0, jnp.where(lane == 0, high, jnp.where(lane == 1, term - high, 0.0)))

    def pack(p, carry):
        for r in range(blk_pp):
            sacc[p, r, :, pl.ds(0, d)] = acc[pick(blks, me, n_dp, blk, p, r)].astype(BF16)
            sacc[p, r, :, pl.ds(d, LANES)] = tail.astype(BF16)
        return carry

    lax.fori_loop(0, n_dp, pack, 0)
    racc[me] = sacc[me]
    for j in range(mb):
        owner, number = origin(secs, sec, mb, act_pp, j)
        for k in range(CHUNKS):
            moved[j, :, k * kd:(k + 1) * kd] = actrecv[k][owner, number]

    def source_of(way, hop, c):
        return 2 * chip_at(pos - step_of[way] * hop) + c

    other = me + 1 - 2 * core

    def project(k):
        hand_over(other, k, own_sem.at[k]).wait_recv()
        for hop in range(1, far + 1):
            for way in range(2):
                if hop <= hops(way, k):
                    hand_over(source_of(way, hop, 1 - core), k, fwd_sem.at[way, hop - 1, k]).wait_recv()
        rows = gath[k, :, :, pl.ds(0, kd)].reshape(length, kd)
        terms = jnp.dot(rows, w[k * kd:(k + 1) * kd, :], preferred_element_type=F32)
        qkv[...] = terms if k == 0 else qkv[...] + terms

    for hop in range(1, far + 1):
        for k in range(CHUNKS):
            for way in range(2):
                if hop > hops(way, k):
                    continue
                source = source_of(way, hop, core)
                gather_copy(way, hop, k, source).wait_recv()
                if hop < hops(way, k):
                    copy = gather_copy(way, hop + 1, k, source)
                    copy.start()
                    sent.append(copy)
                pass_on(source, k, fwd_sem.at[way, hop - 1, k])
            if hop == far and k == 0:
                kv_copy.wait_recv()
                loads["wq"].wait()
            elif hop == far:
                project(k - 1)
        if hop == far - 1:
            blk_copies = []
            for o in range(1, n_dp):
                peer = (me + o) % n_dp
                copy = remote(sacc.at[peer], racc.at[me], blk_sem.at[o - 1], {"dp": peer})
                copy.start()
                blk_copies.append(copy)
    project(CHUNKS - 1)

    loads["rot"].wait()
    parts = gath[CHUNKS - 1, :, :, pl.ds(kd, LANES)].reshape(length, LANES).astype(F32)
    root = jnp.sum(parts, axis=-1, keepdims=True)
    cosine, sine = rot[0] * root, rot[1] * root

    def turned(v):
        return (v * cosine + pltpu.roll(v, hd // 2, 1) * sine).astype(BF16)

    queries = turned(qkv[:, 0:hd])
    keys = turned(qkv[:, hd:2 * hd])
    values = (qkv[:, 2 * hd:3 * hd] * root).astype(BF16)
    scores = lax.dot_general(queries, keys, (((1,), (1,)), ((), ())), preferred_element_type=F32)
    scores = scores * ((d / n_dp) ** (-0.5) / 50.0)
    at_query = lax.broadcasted_iota(jnp.int32, scores.shape, 0)
    at_key = lax.broadcasted_iota(jnp.int32, scores.shape, 1)
    expd = jnp.where(at_key <= at_query, jnp.exp(50.0 * jnp.tanh(scores)), 0.0)
    denominator = jnp.sum(expd, axis=-1, keepdims=True)
    numer = jnp.dot(expd.astype(BF16), values, preferred_element_type=F32)
    attended = (numer / denominator).astype(BF16)

    att[...] = attended.reshape(chips, 2, toks, hd)
    att_copy = remote(att.at[:, 1 - core], att_in, att_sem, partner)
    att_copy.start()
    wo_copy.wait_recv()
    ours = att[:, core].reshape(chips * toks, hd)
    att_copy.wait_recv()
    theirs = att_in[...].reshape(chips * toks, hd)
    even = core == 0
    both = jnp.concatenate([jnp.where(even, ours, theirs), jnp.where(even, theirs, ours)], axis=1)

    def ring_copy(way, step, k):
        return remote(ring_out.at[way, step - 1, k], ring_in.at[way, step - 1, k],
                      ring_sem.at[way, step - 1, k], device(pos + step_of[way]))

    for k in range(CHUNKS):
        terms = jnp.dot(both, wo[:, k * kd:(k + 1) * kd], preferred_element_type=F32)
        part[k] = terms.reshape(chips, toks, kd)
        for way in range(2):
            ring_out[way, 0, k] = part[k, chip_at(pos + step_of[way] * hops(way, k))].astype(BF16)
            copy = ring_copy(way, 1, k)
            copy.start()
            sent.append(copy)
    for step in range(1, far):
        for k in range(CHUNKS):
            for way in range(2):
                left = hops(way, k) - step
                if left < 1:
                    continue
                ring_copy(way, step, k).wait_recv()
                total = part[k, chip_at(pos + step_of[way] * left)] + ring_in[way, step - 1, k].astype(F32)
                ring_out[way, step, k] = total.astype(BF16)
                copy = ring_copy(way, step + 1, k)
                copy.start()
                sent.append(copy)

    for copy in blk_copies:
        copy.wait_recv()
    scale_sum = jnp.sum(racc[:, 0, :, pl.ds(d, LANES)].astype(F32), axis=0)
    factor = n_dp / jnp.sum(jnp.sum(scale_sum, axis=0, keepdims=True), axis=1, keepdims=True)

    def unpack(b, carry):
        owner, number = origin(blks, me, blk, blk_pp, b)
        accout[b] = racc[owner, number, :, pl.ds(0, d)].astype(F32) * factor
        return carry

    lax.fori_loop(0, blk, unpack, 0)

    pieces = []
    for k in range(CHUNKS):
        total = part[k, chip_at(pos)]
        for way in range(2):
            step = hops(way, k)
            ring_copy(way, step, k).wait_recv()
            total = total + ring_in[way, step - 1, k].astype(F32)
        pieces.append(total)
    loads["post"].wait()
    square = sum(jnp.sum(t * t, axis=-1, keepdims=True) for t in pieces)
    scale = lax.rsqrt(square / d + 1e-06)
    for k in range(CHUNKS):
        cols = slice(k * kd, (k + 1) * kd)
        outbuf[0, :, cols] = (
            moved[0, :, cols].astype(F32) + pieces[k] * scale * post[:, cols]
        ).astype(BF16)
    for copy in sum(act_copies, []) + [kv_copy, wo_copy, att_copy] + sent + blk_copies:
        copy.wait_send()


def write_out(moved, accout, outbuf, moved_hbm, newacc_hbm, check_hbm, sems):
    copies = [
        pltpu.make_async_copy(src, dst, sems.at[i])
        for i, (src, dst) in enumerate([(accout, newacc_hbm), (moved, moved_hbm), (outbuf, check_hbm)])
    ]
    for copy in copies:
        copy.start()
    for copy in copies:
        copy.wait()


def make_on_device(n_sec, n_dp):
    def on_device(activations, section_sources, accumulators, block_sources, loss_terms,
                  pre_gain, query_weight, keyval_weight, output_weight, post_gain):
        mb, toks, d = activations.shape
        blk, brows, _ = accumulators.shape
        hd = query_weight.shape[2]
        chips, far, kd, length = n_dp // 2, n_dp // 4, d // CHUNKS, n_dp * toks
        rot = jnp.asarray(rotary_tables(length, hd))
        smem = pltpu.SMEM
        in_hbm = pl.BlockSpec(memory_space=pltpu.HBM)
        vmem = pl.BlockSpec(memory_space=pltpu.VMEM)
        dma = pltpu.SemaphoreType.DMA
        act_pp, blk_pp = mb // n_sec, blk // n_dp
        out_bytes = activations.size * 2 + accumulators.size * 4 + toks * d * 2
        held = pl.pallas_call(
            functools.partial(kernel, (n_sec, n_dp)),
            out_shape=(
                pltpu.VMEM(activations.shape, BF16),
                pltpu.VMEM(accumulators.shape, F32),
                pltpu.VMEM((1, toks, d), BF16),
            ),
            in_specs=[in_hbm] * 11,
            out_specs=(vmem,) * 3,
            scratch_shapes=[
                smem(section_sources.shape, jnp.int32),
                smem(block_sources.shape, jnp.int32),
                smem((1, 1), F32),
                pltpu.VMEM(activations.shape, BF16),
                pltpu.VMEM(accumulators.shape, F32),
                pltpu.VMEM((1, d), F32),
                pltpu.VMEM((1, d), F32),
                pltpu.VMEM(rot.shape, F32),
                pltpu.VMEM((d, 3 * hd), BF16),
                pltpu.VMEM((2 * hd, d), BF16),
                pltpu.VMEM((n_sec, CHUNKS, act_pp, toks, kd), BF16),
                (pltpu.VMEM((n_sec, act_pp, toks, kd), BF16),) * CHUNKS,
                pltpu.VMEM((n_dp, blk_pp, brows, d + LANES), BF16),
                pltpu.VMEM((n_dp, blk_pp, brows, d + LANES), BF16),
                pltpu.VMEM((CHUNKS, n_dp, toks, kd + LANES), BF16),
                pltpu.VMEM((length, 3 * hd), F32),
                pltpu.VMEM((chips, 2, toks, hd), BF16),
                pltpu.VMEM((chips, toks, hd), BF16),
                pltpu.VMEM((CHUNKS, chips, toks, kd), F32),
                pltpu.VMEM((2, far, CHUNKS, toks, kd), BF16),
                pltpu.VMEM((2, far, CHUNKS, toks, kd), BF16),
                dma((11,)),
                dma((n_sec - 1, CHUNKS, 2)),
                dma((2,)),
                dma((2,)),
                dma((n_dp - 1, 2)),
                dma((2, far, CHUNKS, 2)),
                dma((CHUNKS, 2)),
                dma((2, far, CHUNKS, 2)),
                dma((2,)),
                dma((2, far, CHUNKS, 2)),
            ],
            compiler_params=pltpu.CompilerParams(
                collective_id=0, has_side_effects=True, vmem_limit_bytes=VMEM_BYTES - 2**16 - out_bytes
            ),
        )(section_sources, block_sources, loss_terms, activations, accumulators,
          pre_gain, query_weight, keyval_weight, output_weight, post_gain, rot)
        return pl.pallas_call(
            write_out,
            out_shape=(
                jax.ShapeDtypeStruct(activations.shape, BF16),
                jax.ShapeDtypeStruct(accumulators.shape, F32),
                jax.ShapeDtypeStruct((1, toks, d), BF16),
            ),
            in_specs=[vmem] * 3,
            out_specs=(in_hbm,) * 3,
            scratch_shapes=[dma((3,))],
            compiler_params=pltpu.CompilerParams(vmem_limit_bytes=4 * 2**20),
        )(*held)

    return on_device


def solution(mesh):
    placed = (
        P("section", "dp", None),
        P(),
        P("dp", "section", None),
        P(),
        P("section", "dp"),
        P("section", None),
        P("section", None, "dp"),
        P("section", None, "dp"),
        P("section", "dp", None),
        P("section", None),
    )
    return jax.shard_map(
        make_on_device(mesh.shape["section"], mesh.shape["dp"]),
        mesh=mesh,
        in_specs=placed,
        out_specs=(P("section", "dp", None), P("dp", "section", None), P("section", "dp", None)),
        check_vma=False,
    )
```

```python
import functools

import jax
import jax.numpy as jnp
import numpy as np
from jax import lax
from jax.experimental import pallas as pl
from jax.experimental.pallas import tpu as pltpu
from jax.sharding import PartitionSpec as P

LANES = 128
VMEM_BYTES = 67043328
CHUNKS = 6
F32 = jnp.float32
BF16 = jnp.bfloat16


def pick(table, own, groups, per_group, peer, rank):
    def visit(j, carry):
        seen, found = carry
        source = table[peer * per_group + j]
        mine = (source // per_group == own).astype(jnp.int32)
        hit = mine * (seen == rank).astype(jnp.int32)
        return seen + mine, found + hit * (source % per_group)

    zero = jnp.int32(0)
    return lax.fori_loop(0, per_group, visit, (zero, zero), unroll=True)[1]


def origin(table, own, per_group, per_peer, entry):
    owner = table[own * per_group + entry] // per_group
    if per_peer == 1:
        return owner, 0

    def visit(j, seen):
        same = table[own * per_group + j] // per_group == owner
        return seen + same.astype(jnp.int32) * (j < entry).astype(jnp.int32)

    return owner, lax.fori_loop(0, per_group, visit, jnp.int32(0))


def rotary_tables(length, width):
    half = width // 2
    freqs = np.float32(10000.0) ** (np.float32(-2.0) * np.arange(half, dtype=np.float32) / np.float32(width))
    angles = np.arange(length, dtype=np.float32)[:, None] * freqs.astype(np.float32)[None, :]
    cosine, sine = np.cos(angles.astype(np.float64)), np.sin(angles.astype(np.float64))
    return np.stack(
        [np.concatenate([cosine, cosine], 1), np.concatenate([-sine, sine], 1)]
    ).astype(np.float32)


def kernel(
    dims,
    secs_hbm, blks_hbm, loss_hbm, act_hbm, acc_hbm, pre_hbm, wq_hbm, wkv_hbm, wo_hbm, post_hbm, rot_hbm,
    moved, accout, outbuf,
    secs, blks, loss, act, acc, pre, post, rot, w, wo,
    stage, actrecv, sacc, racc,
    gath, qkv, att, att_in, part, ring_in, ring_out,
    load_sem, act_sem, w_sem, wo_sem, blk_sem, ag_sem, own_sem, fwd_sem, att_sem, ring_sem,
):
    n_sec, n_dp = dims
    mb, toks, d = act.shape
    blk, brows, _ = acc.shape
    act_pp, blk_pp = mb // n_sec, blk // n_dp
    chips = n_dp // 2
    far = chips // 2
    kd = d // CHUNKS
    length = n_dp * toks
    hd = wq_hbm.shape[2]
    sec, me = lax.axis_index("section"), lax.axis_index("dp")
    core, chip = me % 2, me // 2
    side, rung = chip % 2, chip // 2
    pos = rung * (1 - side) + (chips - 1 - rung) * side

    def chip_at(p):
        q = (p + 2 * chips) % chips
        s = q // (chips // 2)
        return 2 * (q * (1 - s) + (chips - 1 - q) * s) + s

    def device(p):
        return {"dp": 2 * chip_at(p) + core}

    partner = {"dp": me + 1 - 2 * core}

    def remote(src, dst, sems, dev):
        return pltpu.make_async_remote_copy(
            src_ref=src, dst_ref=dst, send_sem=sems.at[0], recv_sem=sems.at[1],
            device_id=dev, device_id_type=pl.DeviceIdType.MESH,
        )

    barrier = pltpu.get_barrier_semaphore()
    for o in range(1, n_sec):
        pl.semaphore_signal(barrier, inc=1, device_id={"section": (sec + o) % n_sec},
                            device_id_type=pl.DeviceIdType.MESH)
    for near in (device(pos + 1), device(pos - 1), partner):
        pl.semaphore_signal(barrier, inc=1, device_id=near, device_id_type=pl.DeviceIdType.MESH)

    kv_cols = pl.ds(pl.multiple_of(hd + core * hd, LANES), hd)
    q_cols = pl.ds(0, hd)
    wo_rows = pl.ds(pl.multiple_of(core * hd, LANES), hd)
    names = ("secs", "act", "pre", "wkv", "wo", "blks", "loss", "acc", "wq", "rot", "post")
    pairs = [
        (secs_hbm, secs), (act_hbm, act), (pre_hbm, pre), (wkv_hbm.at[0], w.at[:, kv_cols]),
        (wo_hbm.at[0], wo.at[wo_rows]), (blks_hbm, blks), (loss_hbm, loss), (acc_hbm, acc),
        (wq_hbm.at[0], w.at[:, q_cols]), (rot_hbm, rot), (post_hbm, post),
    ]
    loads = {
        name: pltpu.make_async_copy(src, dst, load_sem.at[i])
        for i, (name, (src, dst)) in enumerate(zip(names, pairs))
    }
    for name in names:
        loads[name].start()

    loads["secs"].wait()
    loads["act"].wait()
    for q in range(n_sec):
        for r in range(act_pp):
            block = act[pick(secs, sec, n_sec, mb, q, r)]
            for k in range(CHUNKS):
                stage[q, k, r] = block[:, k * kd:(k + 1) * kd]
    pl.semaphore_wait(barrier, n_sec - 1 + 3)
    act_copies = [[] for _ in range(CHUNKS)]
    for k in range(CHUNKS):
        for o in range(1, n_sec):
            q = (sec + o) % n_sec
            copy = remote(stage.at[q, k], actrecv[k].at[sec], act_sem.at[o - 1, k], {"section": q})
            copy.start()
            act_copies[k].append(copy)
    for k in range(CHUNKS):
        actrecv[k][sec] = stage[sec, k]

    loads["wkv"].wait()
    kv_copy = remote(w.at[:, kv_cols], w.at[:, kv_cols], w_sem, partner)
    kv_copy.start()
    loads["wo"].wait()
    wo_copy = remote(wo.at[wo_rows], wo.at[wo_rows], wo_sem, partner)
    wo_copy.start()
    loads["pre"].wait()

    for name in ("acc", "blks", "loss"):
        loads[name].wait()
    term = jnp.full((brows, LANES), loss[0, 0], F32)
    high = term.astype(BF16).astype(F32)
    lane = lax.broadcasted_iota(jnp.int32, (brows, LANES), 1)
    row = lax.broadcasted_iota(jnp.int32, (brows, LANES), 0)
    tail = jnp.where(row > 0, 0.0, jnp.where(lane == 0, high, jnp.where(lane == 1, term - high, 0.0)))

    def pack(p, carry):
        for r in range(blk_pp):
            sacc[p, r, :, pl.ds(0, d)] = acc[pick(blks, me, n_dp, blk, p, r)].astype(BF16)
            sacc[p, r, :, pl.ds(d, LANES)] = tail.astype(BF16)
        return carry

    lax.fori_loop(0, n_dp, pack, 0)
    racc[me] = sacc[me]

    def hops(way, k):
        return far if (k < CHUNKS // 2) == (way == 0) else far - 1

    step_of = (1, -1)
    sent = []

    def width(k):
        return kd + LANES if k == CHUNKS - 1 else kd

    def block_of(k, source):
        return gath.at[k, source, :, pl.ds(0, width(k))]

    def gather_copy(way, hop, k, source):
        block = block_of(k, source)
        return remote(block, block, ag_sem.at[way, hop - 1, k], device(pos + step_of[way]))

    def hand_over(source, k, sems):
        block = block_of(k, source)
        return remote(block, block, sems, partner)

    def pass_on(source, k, sems):
        copy = hand_over(source, k, sems)
        copy.start()
        sent.append(copy)

    square = jnp.zeros((toks, 1), F32)
    for k in range(CHUNKS):
        for copy in act_copies[k]:
            copy.wait_recv()
        owner, number = origin(secs, sec, mb, act_pp, 0)
        piece = actrecv[k][owner, number].astype(F32)
        square = square + jnp.sum(piece * piece, axis=-1, keepdims=True)
        gath[k, me, :, pl.ds(0, kd)] = (piece * pre[:, k * kd:(k + 1) * kd]).astype(BF16)
        if k == CHUNKS - 1:
            root = jnp.broadcast_to(lax.rsqrt(square / d + 1e-06), (toks, LANES))
            high = root.astype(BF16).astype(F32)
            lane = lax.broadcasted_iota(jnp.int32, (toks, LANES), 1)
            gath[k, me, :, pl.ds(kd, LANES)] = jnp.where(
                lane == 0, high, jnp.where(lane == 1, root - high, 0.0)).astype(BF16)
        for way in range(2):
            copy = gather_copy(way, 1, k, me)
            copy.start()
            sent.append(copy)
        pass_on(me, k, own_sem.at[k])

    def source_of(way, hop, c):
        return 2 * chip_at(pos - step_of[way] * hop) + c

    other = me + 1 - 2 * core

    def project(k):
        hand_over(other, k, own_sem.at[k]).wait_recv()
        for hop in range(1, far + 1):
            for way in range(2):
                if hop <= hops(way, k):
                    hand_over(source_of(way, hop, 1 - core), k, fwd_sem.at[way, hop - 1, k]).wait_recv()
        rows = gath[k, :, :, pl.ds(0, kd)].reshape(length, kd)
        terms = jnp.dot(rows, w[k * kd:(k + 1) * kd, :], preferred_element_type=F32)
        qkv[...] = terms if k == 0 else qkv[...] + terms

    blk_copies = []

    def send_block(peer, slot):
        copy = remote(sacc.at[peer], racc.at[me], blk_sem.at[slot], {"dp": peer})
        copy.start()
        blk_copies.append(copy)

    def send_blocks(places):
        for way, hop in places:
            for c in range(2):
                peer = 2 * chip_at(pos + step_of[way] * hop) + (core + c) % 2
                send_block(peer, 1 + (way * far + hop - 1) * 2 + c)

    send_block(other, 0)
    for hop in range(1, far + 1):
        for k in range(CHUNKS):
            for way in range(2):
                if hop > hops(way, k):
                    continue
                source = source_of(way, hop, core)
                gather_copy(way, hop, k, source).wait_recv()
                if hop < hops(way, k):
                    copy = gather_copy(way, hop + 1, k, source)
                    copy.start()
                    sent.append(copy)
                pass_on(source, k, fwd_sem.at[way, hop - 1, k])
            if hop == far and k == 0:
                kv_copy.wait_recv()
                loads["wq"].wait()
            elif hop == far:
                project(k - 1)
        if hop == far - 1:
            send_blocks([(way, h) for h in range(1, far) for way in range(2)])
    send_blocks([(0, far)])
    project(CHUNKS - 1)

    loads["rot"].wait()
    parts = gath[CHUNKS - 1, :, :, pl.ds(kd, LANES)].reshape(length, LANES).astype(F32)
    root = jnp.sum(parts, axis=-1, keepdims=True)
    cosine, sine = rot[0] * root, rot[1] * root

    def turned(v):
        return (v * cosine + pltpu.roll(v, hd // 2, 1) * sine).astype(BF16)

    queries = turned(qkv[:, 0:hd])
    keys = turned(qkv[:, hd:2 * hd])
    values = (qkv[:, 2 * hd:3 * hd] * root).astype(BF16)
    scores = lax.dot_general(queries, keys, (((1,), (1,)), ((), ())), preferred_element_type=F32)
    scores = scores * ((d / n_dp) ** (-0.5) / 50.0)
    at_query = lax.broadcasted_iota(jnp.int32, scores.shape, 0)
    at_key = lax.broadcasted_iota(jnp.int32, scores.shape, 1)
    expd = jnp.where(at_key <= at_query, jnp.exp(50.0 * jnp.tanh(scores)), 0.0)
    denominator = jnp.sum(expd, axis=-1, keepdims=True)
    numer = jnp.dot(expd.astype(BF16), values, preferred_element_type=F32)
    attended = (numer / denominator).astype(BF16)

    att[...] = attended.reshape(chips, 2, toks, hd)
    att_copy = remote(att.at[:, 1 - core], att_in, att_sem, partner)
    att_copy.start()
    wo_copy.wait_recv()
    ours = att[:, core].reshape(chips * toks, hd)
    att_copy.wait_recv()
    theirs = att_in[...].reshape(chips * toks, hd)
    even = core == 0
    both = jnp.concatenate([jnp.where(even, ours, theirs), jnp.where(even, theirs, ours)], axis=1)

    def ring_copy(way, step, k):
        return remote(ring_out.at[way, step - 1, k], ring_in.at[way, step - 1, k],
                      ring_sem.at[way, step - 1, k], device(pos + step_of[way]))

    for k in range(CHUNKS):
        terms = jnp.dot(both, wo[:, k * kd:(k + 1) * kd], preferred_element_type=F32)
        part[k] = terms.reshape(chips, toks, kd)
        for way in range(2):
            ring_out[way, 0, k] = part[k, chip_at(pos + step_of[way] * hops(way, k))].astype(BF16)
            copy = ring_copy(way, 1, k)
            copy.start()
            sent.append(copy)
    for j in range(mb):
        owner, number = origin(secs, sec, mb, act_pp, j)
        for k in range(CHUNKS):
            moved[j, :, k * kd:(k + 1) * kd] = actrecv[k][owner, number]

    for copy in blk_copies:
        copy.wait_recv()
    scale_sum = jnp.sum(racc[:, 0, :, pl.ds(d, LANES)].astype(F32), axis=0)
    factor = n_dp / jnp.sum(jnp.sum(scale_sum, axis=0, keepdims=True), axis=1, keepdims=True)

    def unpack(b, carry):
        owner, number = origin(blks, me, blk, blk_pp, b)
        accout[b] = racc[owner, number, :, pl.ds(0, d)].astype(F32) * factor
        return carry

    lax.fori_loop(0, blk, unpack, 0)

    for step in range(1, far):
        for k in range(CHUNKS):
            for way in range(2):
                left = hops(way, k) - step
                if left < 1:
                    continue
                ring_copy(way, step, k).wait_recv()
                total = part[k, chip_at(pos + step_of[way] * left)] + ring_in[way, step - 1, k].astype(F32)
                ring_out[way, step, k] = total.astype(BF16)
                copy = ring_copy(way, step + 1, k)
                copy.start()
                sent.append(copy)

    pieces = []
    for k in range(CHUNKS):
        total = part[k, chip_at(pos)]
        for way in range(2):
            step = hops(way, k)
            ring_copy(way, step, k).wait_recv()
            total = total + ring_in[way, step - 1, k].astype(F32)
        pieces.append(total)
    loads["post"].wait()
    square = sum(jnp.sum(t * t, axis=-1, keepdims=True) for t in pieces)
    scale = lax.rsqrt(square / d + 1e-06)
    for k in range(CHUNKS):
        cols = slice(k * kd, (k + 1) * kd)
        outbuf[0, :, cols] = (
            moved[0, :, cols].astype(F32) + pieces[k] * scale * post[:, cols]
        ).astype(BF16)
    for copy in sum(act_copies, []) + [kv_copy, wo_copy, att_copy] + sent + blk_copies:
        copy.wait_send()


def write_out(moved, accout, outbuf, moved_hbm, newacc_hbm, check_hbm, sems):
    copies = [
        pltpu.make_async_copy(src, dst, sems.at[i])
        for i, (src, dst) in enumerate([(accout, newacc_hbm), (moved, moved_hbm), (outbuf, check_hbm)])
    ]
    for copy in copies:
        copy.start()
    for copy in copies:
        copy.wait()


def make_on_device(n_sec, n_dp):
    def on_device(activations, section_sources, accumulators, block_sources, loss_terms,
                  pre_gain, query_weight, keyval_weight, output_weight, post_gain):
        mb, toks, d = activations.shape
        blk, brows, _ = accumulators.shape
        hd = query_weight.shape[2]
        chips, far, kd, length = n_dp // 2, n_dp // 4, d // CHUNKS, n_dp * toks
        rot = jnp.asarray(rotary_tables(length, hd))
        smem = pltpu.SMEM
        in_hbm = pl.BlockSpec(memory_space=pltpu.HBM)
        vmem = pl.BlockSpec(memory_space=pltpu.VMEM)
        dma = pltpu.SemaphoreType.DMA
        act_pp, blk_pp = mb // n_sec, blk // n_dp
        out_bytes = activations.size * 2 + accumulators.size * 4 + toks * d * 2
        held = pl.pallas_call(
            functools.partial(kernel, (n_sec, n_dp)),
            out_shape=(
                pltpu.VMEM(activations.shape, BF16),
                pltpu.VMEM(accumulators.shape, F32),
                pltpu.VMEM((1, toks, d), BF16),
            ),
            in_specs=[in_hbm] * 11,
            out_specs=(vmem,) * 3,
            scratch_shapes=[
                smem(section_sources.shape, jnp.int32),
                smem(block_sources.shape, jnp.int32),
                smem((1, 1), F32),
                pltpu.VMEM(activations.shape, BF16),
                pltpu.VMEM(accumulators.shape, F32),
                pltpu.VMEM((1, d), F32),
                pltpu.VMEM((1, d), F32),
                pltpu.VMEM(rot.shape, F32),
                pltpu.VMEM((d, 3 * hd), BF16),
                pltpu.VMEM((2 * hd, d), BF16),
                pltpu.VMEM((n_sec, CHUNKS, act_pp, toks, kd), BF16),
                (pltpu.VMEM((n_sec, act_pp, toks, kd), BF16),) * CHUNKS,
                pltpu.VMEM((n_dp, blk_pp, brows, d + LANES), BF16),
                pltpu.VMEM((n_dp, blk_pp, brows, d + LANES), BF16),
                pltpu.VMEM((CHUNKS, n_dp, toks, kd + LANES), BF16),
                pltpu.VMEM((length, 3 * hd), F32),
                pltpu.VMEM((chips, 2, toks, hd), BF16),
                pltpu.VMEM((chips, toks, hd), BF16),
                pltpu.VMEM((CHUNKS, chips, toks, kd), F32),
                pltpu.VMEM((2, far, CHUNKS, toks, kd), BF16),
                pltpu.VMEM((2, far, CHUNKS, toks, kd), BF16),
                dma((11,)),
                dma((n_sec - 1, CHUNKS, 2)),
                dma((2,)),
                dma((2,)),
                dma((1 + 4 * far, 2)),
                dma((2, far, CHUNKS, 2)),
                dma((CHUNKS, 2)),
                dma((2, far, CHUNKS, 2)),
                dma((2,)),
                dma((2, far, CHUNKS, 2)),
            ],
            compiler_params=pltpu.CompilerParams(
                collective_id=0, has_side_effects=True, vmem_limit_bytes=VMEM_BYTES - 2**16 - out_bytes
            ),
        )(section_sources, block_sources, loss_terms, activations, accumulators,
          pre_gain, query_weight, keyval_weight, output_weight, post_gain, rot)
        return pl.pallas_call(
            write_out,
            out_shape=(
                jax.ShapeDtypeStruct(activations.shape, BF16),
                jax.ShapeDtypeStruct(accumulators.shape, F32),
                jax.ShapeDtypeStruct((1, toks, d), BF16),
            ),
            in_specs=[vmem] * 3,
            out_specs=(in_hbm,) * 3,
            scratch_shapes=[dma((3,))],
            compiler_params=pltpu.CompilerParams(vmem_limit_bytes=4 * 2**20),
        )(*held)

    return on_device


def solution(mesh):
    placed = (
        P("section", "dp", None),
        P(),
        P("dp", "section", None),
        P(),
        P("section", "dp"),
        P("section", None),
        P("section", None, "dp"),
        P("section", None, "dp"),
        P("section", "dp", None),
        P("section", None),
    )
    return jax.shard_map(
        make_on_device(mesh.shape["section"], mesh.shape["dp"]),
        mesh=mesh,
        in_specs=placed,
        out_specs=(P("section", "dp", None), P("dp", "section", None), P("section", "dp", None)),
        check_vma=False,
    )
```

```python
import functools

import jax
import jax.numpy as jnp
import numpy as np
from jax import lax
from jax.experimental import pallas as pl
from jax.experimental.pallas import tpu as pltpu
from jax.sharding import PartitionSpec as P

LANES = 128
VMEM_BYTES = 67043328
CHUNKS = 6
F32 = jnp.float32
BF16 = jnp.bfloat16


def pick(table, own, groups, per_group, peer, rank):
    def visit(j, carry):
        seen, found = carry
        source = table[peer * per_group + j]
        mine = (source // per_group == own).astype(jnp.int32)
        hit = mine * (seen == rank).astype(jnp.int32)
        return seen + mine, found + hit * (source % per_group)

    zero = jnp.int32(0)
    return lax.fori_loop(0, per_group, visit, (zero, zero), unroll=True)[1]


def origin(table, own, per_group, per_peer, entry):
    owner = table[own * per_group + entry] // per_group
    if per_peer == 1:
        return owner, 0

    def visit(j, seen):
        same = table[own * per_group + j] // per_group == owner
        return seen + same.astype(jnp.int32) * (j < entry).astype(jnp.int32)

    return owner, lax.fori_loop(0, per_group, visit, jnp.int32(0))


def rotary_tables(length, width):
    half = width // 2
    freqs = np.float32(10000.0) ** (np.float32(-2.0) * np.arange(half, dtype=np.float32) / np.float32(width))
    angles = np.arange(length, dtype=np.float32)[:, None] * freqs.astype(np.float32)[None, :]
    cosine, sine = np.cos(angles.astype(np.float64)), np.sin(angles.astype(np.float64))
    return np.stack(
        [np.concatenate([cosine, cosine], 1), np.concatenate([-sine, sine], 1)]
    ).astype(np.float32)


def kernel(
    dims,
    secs_hbm, blks_hbm, loss_hbm, act_hbm, acc_hbm, pre_hbm, wq_hbm, wkv_hbm, wo_hbm, post_hbm, rot_hbm,
    moved, accout, outbuf,
    secs, blks, loss, act, acc, pre, post, rot, w, wo,
    stage, actrecv, sacc, racc,
    gath, qkv, att, att_in, part, ring_in, ring_out,
    load_sem, act_out, act_sem, w_sem, wo_sem, blk_sem, ag_out, ag_sem, fwd_sem, att_sem, ring_done, ring_sem,
):
    n_sec, n_dp = dims
    mb, toks, d = act.shape
    blk, brows, _ = acc.shape
    act_pp, blk_pp = mb // n_sec, blk // n_dp
    chips = n_dp // 2
    far = chips // 2
    kd = d // CHUNKS
    length = n_dp * toks
    hd = wq_hbm.shape[2]
    sec, me = lax.axis_index("section"), lax.axis_index("dp")
    core, chip = me % 2, me // 2
    side, rung = chip % 2, chip // 2
    pos = rung * (1 - side) + (chips - 1 - rung) * side

    def chip_at(p):
        q = (p + 2 * chips) % chips
        s = q // (chips // 2)
        return 2 * (q * (1 - s) + (chips - 1 - q) * s) + s

    def device(p):
        return {"dp": 2 * chip_at(p) + core}

    partner = {"dp": me + 1 - 2 * core}

    def remote(src, dst, send_sem, recv_sem, dev):
        return pltpu.make_async_remote_copy(
            src_ref=src, dst_ref=dst, send_sem=send_sem, recv_sem=recv_sem,
            device_id=dev, device_id_type=pl.DeviceIdType.MESH,
        )

    barrier = pltpu.get_barrier_semaphore()
    for o in range(1, n_sec):
        pl.semaphore_signal(barrier, inc=1, device_id={"section": (sec + o) % n_sec},
                            device_id_type=pl.DeviceIdType.MESH)
    for near in (device(pos + 1), device(pos - 1), partner):
        pl.semaphore_signal(barrier, inc=1, device_id=near, device_id_type=pl.DeviceIdType.MESH)

    kv_cols = pl.ds(pl.multiple_of(hd + core * hd, LANES), hd)
    q_cols = pl.ds(0, hd)
    wo_rows = pl.ds(pl.multiple_of(core * hd, LANES), hd)
    names = ("secs", "act", "pre", "wkv", "wo", "blks", "loss", "acc", "wq", "rot", "post")
    pairs = [
        (secs_hbm, secs), (act_hbm, act), (pre_hbm, pre), (wkv_hbm.at[0], w.at[:, kv_cols]),
        (wo_hbm.at[0], wo.at[wo_rows]), (blks_hbm, blks), (loss_hbm, loss), (acc_hbm, acc),
        (wq_hbm.at[0], w.at[:, q_cols]), (rot_hbm, rot), (post_hbm, post),
    ]
    loads = {
        name: pltpu.make_async_copy(src, dst, load_sem.at[i])
        for i, (name, (src, dst)) in enumerate(zip(names, pairs))
    }
    for name in names:
        loads[name].start()

    loads["secs"].wait()
    loads["act"].wait()
    for q in range(n_sec):
        for r in range(act_pp):
            block = act[pick(secs, sec, n_sec, mb, q, r)]
            for k in range(CHUNKS):
                stage[q, k, r] = block[:, k * kd:(k + 1) * kd]
    pl.semaphore_wait(barrier, n_sec - 1 + 3)
    act_copies = [[] for _ in range(CHUNKS)]
    for k in range(CHUNKS):
        for o in range(1, n_sec):
            q = (sec + o) % n_sec
            copy = remote(stage.at[q, k], actrecv[k].at[sec], act_out.at[o - 1], act_sem.at[o - 1, k], {"section": q})
            copy.start()
            act_copies[k].append(copy)
    for k in range(CHUNKS):
        actrecv[k][sec] = stage[sec, k]

    loads["wkv"].wait()
    kv_copy = remote(w.at[:, kv_cols], w.at[:, kv_cols], w_sem.at[0], w_sem.at[1], partner)
    kv_copy.start()
    loads["wo"].wait()
    wo_copy = remote(wo.at[wo_rows], wo.at[wo_rows], wo_sem.at[0], wo_sem.at[1], partner)
    wo_copy.start()
    loads["pre"].wait()

    for name in ("acc", "blks", "loss"):
        loads[name].wait()
    term = jnp.full((brows, LANES), loss[0, 0], F32)
    high = term.astype(BF16).astype(F32)
    lane = lax.broadcasted_iota(jnp.int32, (brows, LANES), 1)
    row = lax.broadcasted_iota(jnp.int32, (brows, LANES), 0)
    tail = jnp.where(row > 0, 0.0, jnp.where(lane == 0, high, jnp.where(lane == 1, term - high, 0.0)))

    def pack(p, carry):
        for r in range(blk_pp):
            sacc[p, r, :, pl.ds(0, d)] = acc[pick(blks, me, n_dp, blk, p, r)].astype(BF16)
            sacc[p, r, :, pl.ds(d, LANES)] = tail.astype(BF16)
        return carry

    lax.fori_loop(0, n_dp, pack, 0)
    racc[me] = sacc[me]

    def hops(way, k):
        return far if (k < CHUNKS // 2) == (way == 0) else far - 1

    step_of = (1, -1)

    def width(k):
        return kd + LANES if k == CHUNKS - 1 else kd

    def blocks_of(k, c, places):
        return gath.at[k, c, places, :, pl.ds(0, width(k))]

    def gather_copy(way, hop, k, place):
        block = blocks_of(k, core, place)
        return remote(block, block, ag_out.at[k], ag_sem.at[way, hop - 1, k], device(pos + step_of[way]))

    def pass_on(place, k):
        block = blocks_of(k, core, place)
        remote(block, block, fwd_sem.at[0, k], fwd_sem.at[1, k], partner).start()

    square = jnp.zeros((toks, 1), F32)
    for k in range(CHUNKS):
        for copy in act_copies[k]:
            copy.wait_recv()
        owner, number = origin(secs, sec, mb, act_pp, 0)
        piece = actrecv[k][owner, number].astype(F32)
        square = square + jnp.sum(piece * piece, axis=-1, keepdims=True)
        gath[k, core, chip, :, pl.ds(0, kd)] = (piece * pre[:, k * kd:(k + 1) * kd]).astype(BF16)
        if k == CHUNKS - 1:
            root = jnp.broadcast_to(lax.rsqrt(square / d + 1e-06), (toks, LANES))
            high = root.astype(BF16).astype(F32)
            lane = lax.broadcasted_iota(jnp.int32, (toks, LANES), 1)
            gath[k, core, chip, :, pl.ds(kd, LANES)] = jnp.where(
                lane == 0, high, jnp.where(lane == 1, root - high, 0.0)).astype(BF16)
        for way in range(2):
            gather_copy(way, 1, k, chip).start()
        pass_on(chip, k)

    other = me + 1 - 2 * core

    def project(k):
        block = blocks_of(k, 1 - core, slice(None))
        remote(block, block, fwd_sem.at[0, k], fwd_sem.at[1, k], partner).wait_recv()
        rows = gath[k, :, :, :, pl.ds(0, kd)].reshape(length, kd)
        terms = jnp.dot(rows, w[k * kd:(k + 1) * kd, :], preferred_element_type=F32)
        qkv[...] = terms if k == 0 else qkv[...] + terms

    def send_block(peer):
        remote(sacc.at[peer], racc.at[me], blk_sem.at[0], blk_sem.at[1], {"dp": peer}).start()

    def send_blocks(places):
        for way, hop in places:
            for c in range(2):
                send_block(2 * chip_at(pos + step_of[way] * hop) + (core + c) % 2)

    send_block(other)
    for hop in range(1, far + 1):
        for k in range(CHUNKS):
            for way in range(2):
                if hop > hops(way, k):
                    continue
                place = chip_at(pos - step_of[way] * hop)
                gather_copy(way, hop, k, place).wait_recv()
                if hop < hops(way, k):
                    gather_copy(way, hop + 1, k, place).start()
                pass_on(place, k)
            if hop == far and k == 0:
                kv_copy.wait_recv()
                loads["wq"].wait()
            elif hop == far:
                project(k - 1)
        if hop == far - 1:
            send_blocks([(way, h) for h in range(1, far) for way in range(2)])
    send_blocks([(0, far)])
    project(CHUNKS - 1)

    loads["rot"].wait()
    parts = gath[CHUNKS - 1, :, :, :, pl.ds(kd, LANES)].reshape(length, LANES).astype(F32)
    root = jnp.sum(parts, axis=-1, keepdims=True)
    cosine, sine = rot[0] * root, rot[1] * root

    def turned(v):
        return (v * cosine + pltpu.roll(v, hd // 2, 1) * sine).astype(BF16)

    def token_at(shape, dim):
        row = lax.broadcasted_iota(jnp.int32, shape, dim)
        block = row // toks
        return (block % chips * 2 + block // chips) * toks + row % toks

    queries = turned(qkv[:, 0:hd])
    keys = turned(qkv[:, hd:2 * hd])
    values = (qkv[:, 2 * hd:3 * hd] * root).astype(BF16)
    scores = lax.dot_general(queries, keys, (((1,), (1,)), ((), ())), preferred_element_type=F32)
    scores = scores * ((d / n_dp) ** (-0.5) / 50.0)
    expd = jnp.where(token_at((1, length), 1) <= token_at((length, 1), 0), jnp.exp(50.0 * jnp.tanh(scores)), 0.0)
    denominator = jnp.sum(expd, axis=-1, keepdims=True)
    numer = jnp.dot(expd.astype(BF16), values, preferred_element_type=F32)
    attended = (numer / denominator).astype(BF16)

    att[...] = attended.reshape(2, chips, toks, hd)
    att_copy = remote(att.at[1 - core], att_in, att_sem.at[0], att_sem.at[1], partner)
    att_copy.start()
    wo_copy.wait_recv()
    ours = att[core].reshape(chips * toks, hd)
    att_copy.wait_recv()
    theirs = att_in[...].reshape(chips * toks, hd)
    even = core == 0
    both = jnp.concatenate([jnp.where(even, ours, theirs), jnp.where(even, theirs, ours)], axis=1)

    def ring_copy(way, step, k):
        return remote(ring_out.at[k, way * far + step - 1], ring_in.at[k, way * far + step - 1],
                      ring_done.at[k], ring_sem.at[way, step - 1, k], device(pos + step_of[way]))

    for k in range(CHUNKS):
        terms = jnp.dot(both, wo[:, k * kd:(k + 1) * kd], preferred_element_type=F32)
        part[k] = terms.reshape(chips, toks, kd)
        for way in range(2):
            ring_out[k, way * far] = part[k, chip_at(pos + step_of[way] * hops(way, k))].astype(BF16)
            ring_copy(way, 1, k).start()
    for j in range(mb):
        owner, number = origin(secs, sec, mb, act_pp, j)
        for k in range(CHUNKS):
            moved[j, :, k * kd:(k + 1) * kd] = actrecv[k][owner, number]

    others = pl.ds(0, n_dp - 1)
    all_blocks = remote(sacc.at[others], racc.at[others], blk_sem.at[0], blk_sem.at[1], partner)
    all_blocks.wait_recv()
    scale_sum = jnp.sum(racc[:, 0, :, pl.ds(d, LANES)].astype(F32), axis=0)
    factor = n_dp / jnp.sum(jnp.sum(scale_sum, axis=0, keepdims=True), axis=1, keepdims=True)

    def unpack(b, carry):
        owner, number = origin(blks, me, blk, blk_pp, b)
        accout[b] = racc[owner, number, :, pl.ds(0, d)].astype(F32) * factor
        return carry

    lax.fori_loop(0, blk, unpack, 0)

    for step in range(1, far):
        for k in range(CHUNKS):
            for way in range(2):
                left = hops(way, k) - step
                if left < 1:
                    continue
                ring_copy(way, step, k).wait_recv()
                total = part[k, chip_at(pos + step_of[way] * left)] + ring_in[k, way * far + step - 1].astype(F32)
                ring_out[k, way * far + step] = total.astype(BF16)
                ring_copy(way, step + 1, k).start()

    pieces = []
    for k in range(CHUNKS):
        total = part[k, chip_at(pos)]
        for way in range(2):
            step = hops(way, k)
            ring_copy(way, step, k).wait_recv()
            total = total + ring_in[k, way * far + step - 1].astype(F32)
        pieces.append(total)
    loads["post"].wait()
    square = sum(jnp.sum(t * t, axis=-1, keepdims=True) for t in pieces)
    scale = lax.rsqrt(square / d + 1e-06)
    for k in range(CHUNKS):
        cols = slice(k * kd, (k + 1) * kd)
        outbuf[0, :, cols] = (
            moved[0, :, cols].astype(F32) + pieces[k] * scale * post[:, cols]
        ).astype(BF16)
    for copy in (kv_copy, wo_copy, att_copy, all_blocks):
        copy.wait_send()
    for o in range(1, n_sec):
        q = (sec + o) % n_sec
        remote(stage.at[q], stage.at[q], act_out.at[o - 1], act_sem.at[o - 1, 0], {"section": q}).wait_send()
    for k in range(CHUNKS):
        for places, sem in ((slice(None), fwd_sem.at[0, k]), (pl.ds(0, chips - 1), ag_out.at[k])):
            block = blocks_of(k, core, places)
            remote(block, block, sem, fwd_sem.at[1, k], partner).wait_send()
        block = ring_out.at[k, pl.ds(0, chips - 1)]
        remote(block, block, ring_done.at[k], fwd_sem.at[1, k], partner).wait_send()


def write_out(moved, accout, outbuf, moved_hbm, newacc_hbm, check_hbm, sems):
    copies = [
        pltpu.make_async_copy(src, dst, sems.at[i])
        for i, (src, dst) in enumerate([(accout, newacc_hbm), (moved, moved_hbm), (outbuf, check_hbm)])
    ]
    for copy in copies:
        copy.start()
    for copy in copies:
        copy.wait()


def make_on_device(n_sec, n_dp):
    def on_device(activations, section_sources, accumulators, block_sources, loss_terms,
                  pre_gain, query_weight, keyval_weight, output_weight, post_gain):
        mb, toks, d = activations.shape
        blk, brows, _ = accumulators.shape
        hd = query_weight.shape[2]
        chips, far, kd, length = n_dp // 2, n_dp // 4, d // CHUNKS, n_dp * toks
        order = np.arange(length).reshape(chips, 2, toks).transpose(1, 0, 2).reshape(-1)
        rot = jnp.asarray(rotary_tables(length, hd)[:, order])
        smem = pltpu.SMEM
        in_hbm = pl.BlockSpec(memory_space=pltpu.HBM)
        vmem = pl.BlockSpec(memory_space=pltpu.VMEM)
        dma = pltpu.SemaphoreType.DMA
        act_pp, blk_pp = mb // n_sec, blk // n_dp
        out_bytes = activations.size * 2 + accumulators.size * 4 + toks * d * 2
        held = pl.pallas_call(
            functools.partial(kernel, (n_sec, n_dp)),
            out_shape=(
                pltpu.VMEM(activations.shape, BF16),
                pltpu.VMEM(accumulators.shape, F32),
                pltpu.VMEM((1, toks, d), BF16),
            ),
            in_specs=[in_hbm] * 11,
            out_specs=(vmem,) * 3,
            scratch_shapes=[
                smem(section_sources.shape, jnp.int32),
                smem(block_sources.shape, jnp.int32),
                smem((1, 1), F32),
                pltpu.VMEM(activations.shape, BF16),
                pltpu.VMEM(accumulators.shape, F32),
                pltpu.VMEM((1, d), F32),
                pltpu.VMEM((1, d), F32),
                pltpu.VMEM(rot.shape, F32),
                pltpu.VMEM((d, 3 * hd), BF16),
                pltpu.VMEM((2 * hd, d), BF16),
                pltpu.VMEM((n_sec, CHUNKS, act_pp, toks, kd), BF16),
                (pltpu.VMEM((n_sec, act_pp, toks, kd), BF16),) * CHUNKS,
                pltpu.VMEM((n_dp, blk_pp, brows, d + LANES), BF16),
                pltpu.VMEM((n_dp, blk_pp, brows, d + LANES), BF16),
                pltpu.VMEM((CHUNKS, 2, chips, toks, kd + LANES), BF16),
                pltpu.VMEM((length, 3 * hd), F32),
                pltpu.VMEM((2, chips, toks, hd), BF16),
                pltpu.VMEM((chips, toks, hd), BF16),
                pltpu.VMEM((CHUNKS, chips, toks, kd), F32),
                pltpu.VMEM((CHUNKS, 2 * far, toks, kd), BF16),
                pltpu.VMEM((CHUNKS, 2 * far, toks, kd), BF16),
                dma((11,)),
                dma((n_sec - 1,)),
                dma((n_sec - 1, CHUNKS)),
                dma((2,)),
                dma((2,)),
                dma((2,)),
                dma((CHUNKS,)),
                dma((2, far, CHUNKS)),
                dma((2, CHUNKS)),
                dma((2,)),
                dma((CHUNKS,)),
                dma((2, far, CHUNKS)),
            ],
            compiler_params=pltpu.CompilerParams(
                collective_id=0, has_side_effects=True, vmem_limit_bytes=VMEM_BYTES - 2**16 - out_bytes
            ),
        )(section_sources, block_sources, loss_terms, activations, accumulators,
          pre_gain, query_weight, keyval_weight, output_weight, post_gain, rot)
        return pl.pallas_call(
            write_out,
            out_shape=(
                jax.ShapeDtypeStruct(activations.shape, BF16),
                jax.ShapeDtypeStruct(accumulators.shape, F32),
                jax.ShapeDtypeStruct((1, toks, d), BF16),
            ),
            in_specs=[vmem] * 3,
            out_specs=(in_hbm,) * 3,
            scratch_shapes=[dma((3,))],
            compiler_params=pltpu.CompilerParams(vmem_limit_bytes=4 * 2**20),
        )(*held)

    return on_device


def solution(mesh):
    placed = (
        P("section", "dp", None),
        P(),
        P("dp", "section", None),
        P(),
        P("section", "dp"),
        P("section", None),
        P("section", None, "dp"),
        P("section", None, "dp"),
        P("section", "dp", None),
        P("section", None),
    )
    return jax.shard_map(
        make_on_device(mesh.shape["section"], mesh.shape["dp"]),
        mesh=mesh,
        in_specs=placed,
        out_specs=(P("section", "dp", None), P("dp", "section", None), P("section", "dp", None)),
        check_vma=False,
    )
```
